32 devices in a mesh: freq: 4 (over y, core), stn: 8 (over z, x).
Axes of the slice: x: 2, y: 2, z: 4, core: 2. Of those that a mesh axis runs over, the one named last changes fastest.
Arguments:
- samples: bfloat16 [4, 256, 24, 2, 128], P('freq', 'stn'), may hold values from -8 to 8, as said below
- window: float32 [128], replicated, may hold values from 0.1 to 1
- group_of_device: int32 [8], replicated, may hold values from 0 to 7, each once
- owner_map: int32 [8, 8], replicated, may hold values from 0 to 7, as said below
Outputs:
- owned: bfloat16 [2, 32, 8, 8, 1024], P(None, None, 'stn', 'freq')
The draws below stay inside these ranges and needn't reach their ends.
Inputs may be any that keep to these rules, and one draw needn't show every extreme that they name: `samples`: samples are finite and bounded. Every row and every column of owner_map names each stn index exactly once.
All inputs are finite; a program needn't handle non-finite values.
Results may differ from the reference program's by a relative error of at most 0.0065.
Values may be sent and summed in bfloat16 or wider, within the bound.
A program may use at most 64 MiB of HBM per device.

```python
import math
import jax
import jax.numpy as jnp
from jax import lax

FFT_LEN = 128
AVG = 16
SPEC = 24
GRP_IN = 32
CH_OUT = 8
GROUPS = 8
BANDS = 4
INPUTS = 256
CHANNELS = 32


def draw_samples(key, part):
    sky_sources = 32
    keys = jax.random.split(key, 3)
    shape = (BANDS, INPUTS, SPEC, 2, FFT_LEN)
    gains = jax.random.normal(keys[1], (INPUTS, sky_sources), jnp.float32)
    signals = jax.random.normal(keys[2], (BANDS, sky_sources, SPEC, 2, FFT_LEN), jnp.float32)
    common = jnp.einsum('ik,bktrn->bitrn', gains, signals) / math.sqrt(sky_sources)
    noise = jax.random.normal(keys[0], shape, jnp.float32)
    total = 0.55 * noise + common
    return jnp.clip(total, -8.0, 8.0).astype(jnp.bfloat16)


def draw_owner_map(key, part):
    keys = jax.random.split(key, 3)
    row_shift = jax.random.permutation(keys[0], GROUPS)
    col_shift = jax.random.permutation(keys[1], GROUPS)
    labels = jax.random.permutation(keys[2], GROUPS)
    return labels[(row_shift[:, None] + col_shift[None, :]) % GROUPS].astype(jnp.int32)


def setup_inputs(seed: int = 0) -> dict:
    key_of = jax.random.split(jax.random.key(seed), 5)
    return {
        "samples": draw_samples(jax.random.fold_in(key_of[4], 71), 0),
        "window": jnp.clip(jnp.exp(jax.random.uniform(key_of[1], (FFT_LEN,), jnp.float32, math.log(0.1), math.log(1.0))), 0.1, 1.0),
        "group_of_device": jax.random.permutation(key_of[2], GROUPS).astype(jnp.int32),
        "owner_map": draw_owner_map(jax.random.fold_in(key_of[4], 71), 0),
    }


def channel_matrix(window):
    length = window.shape[0]
    index = jnp.arange(length, dtype=jnp.int32)
    product = index[:, None] * index[None, :] % length
    theta = product.astype(jnp.float32) * (2.0 * math.pi / length)
    weights = window[:, None] / math.sqrt(length)
    cosine = weights * jnp.cos(theta)
    sine = weights * jnp.sin(theta)
    upper = jnp.concatenate([cosine, -sine], axis=1)
    lower = jnp.concatenate([sine, cosine], axis=1)
    return jnp.concatenate([upper, lower], axis=0)

def split_matrix(matrix):
    high = matrix.astype(jnp.bfloat16)
    low = (matrix - high.astype(jnp.float32)).astype(jnp.bfloat16)
    return (high, low)

def channelize(block, high, low):
    rows = block.shape[0]
    flat = block.reshape(rows * SPEC, 2 * FFT_LEN)
    spectra = jnp.dot(flat, high, preferred_element_type=jnp.float32) + jnp.dot(flat, low, preferred_element_type=jnp.float32)
    spectra = spectra.astype(jnp.bfloat16).reshape(rows, SPEC, 2, CH_OUT, AVG)
    return spectra.transpose(3, 0, 2, 1, 4).reshape(CH_OUT, rows, 2 * SPEC * AVG)

def reference(samples, window, group_of_device, owner_map):
    high, low = split_matrix(channel_matrix(window))
    order = jnp.arange(GROUPS, dtype=jnp.int32)
    dev_of_group = jnp.zeros((GROUPS,), jnp.int32).at[group_of_device].set(order)
    grouped = samples.reshape(BANDS, GROUPS, GRP_IN, SPEC, 2, FFT_LEN)
    grouped = jnp.take(grouped, dev_of_group, axis=1).reshape(BANDS, INPUTS, SPEC, 2, FFT_LEN)
    column_for = jnp.zeros((GROUPS, GROUPS), jnp.int32).at[order[:, None], owner_map].set(jnp.broadcast_to(order[None, :], (GROUPS, GROUPS)))

    def one_band(band):
        spectra = channelize(band, high, low).astype(jnp.float32)
        half = spectra.shape[2] // 2
        swapped = jnp.concatenate([spectra[..., half:], -spectra[..., :half]], axis=-1)
        stacked = jnp.stack([spectra, swapped])
        vis = jnp.einsum('pcak,cbk->pcab', stacked, spectra)
        vis = (vis * (1.0 / (AVG * SPEC))).astype(jnp.bfloat16)
        vis = vis.reshape(2, CH_OUT, GROUPS, GRP_IN, GROUPS, GRP_IN).transpose(0, 1, 2, 4, 3, 5)
        vis = vis.reshape(2, CH_OUT, GROUPS, GROUPS, GRP_IN * GRP_IN)
        picked = jnp.take_along_axis(vis, column_for[None, None, :, :, None], axis=3)
        return picked.transpose(0, 1, 3, 2, 4)
    result = lax.map(one_band, grouped)
    result = result.transpose(1, 0, 2, 3, 4, 5)
    return result.reshape(2, CHANNELS, GROUPS, GROUPS, GRP_IN * GRP_IN)
```

```python
import functools
import math

import jax
import jax.numpy as jnp
import numpy as np
from jax import lax
from jax.experimental import pallas as pl
from jax.experimental.pallas import tpu as pltpu
from jax.sharding import PartitionSpec as P

AVG = 16
LANES = 128
MESH = pl.DeviceIdType.MESH


def swap_blocks(blocks, width):
    blocks = list(blocks)
    count = len(blocks)
    lane = lax.broadcasted_iota(jnp.int32, blocks[0].shape, 1) // width
    step = count // 2
    while step:
        upper = (lane // step) % 2 == 1
        for i in range(count):
            if (i // step) % 2 == 0:
                u, v = blocks[i], blocks[i + step]
                shift = step * width
                blocks[i] = jnp.where(upper, pltpu.roll(v, shift, 1), u)
                blocks[i + step] = jnp.where(upper, v, pltpu.roll(u, LANES - shift, 1))
        step //= 2
    return blocks


def kernel(
    nf, ns, rows, spec,
    x_ref, w_ref, cos_ref, sin_ref, god_ref, own_ref,
    out_ref,
    xf, send1, held, left, vis, tiles, mixed, send2, dev_of, table,
    ssem1, rsem1, ssem2, rsem2,
):
    length = LANES
    ch_out = length // AVG
    spread = ns // ch_out
    rpf = ns // nf
    fl_count = ch_out // rpf
    half = spec * AVG
    b = lax.axis_index("freq")
    me = lax.axis_index("stn")
    total = nf * ns
    rank = b * ns + me

    barrier = pltpu.get_barrier_semaphore()

    def greet(off, carry):
        other = lax.rem(rank + off, total)
        pl.semaphore_signal(
            barrier, inc=1, device_id=(other // ns, lax.rem(other, ns)), device_id_type=MESH
        )
        return carry

    lax.fori_loop(1, total, greet, 0)

    weights = jnp.broadcast_to(w_ref[...], (length, length)).T * (1.0 / math.sqrt(length))
    cosine = weights * cos_ref[...]
    sine = weights * sin_ref[...]
    matrix = jnp.concatenate(
        [jnp.concatenate([cosine, -sine], axis=1), jnp.concatenate([sine, cosine], axis=1)], axis=0
    )
    high = matrix.astype(jnp.bfloat16)
    low = (matrix - high.astype(jnp.float32)).astype(jnp.bfloat16)

    xf[...] = x_ref[...].astype(jnp.float32)
    for th in range(spec // ch_out):
        parts = []
        for t in range(th * ch_out, (th + 1) * ch_out):
            re = xf[pl.ds(2 * t, rows, stride=2 * spec), :]
            im = xf[pl.ds(2 * t + 1, rows, stride=2 * spec), :]
            parts.append(jnp.concatenate([re, im], axis=1).astype(jnp.bfloat16))
        flat = jnp.concatenate(parts, axis=0)
        spectra = jnp.dot(flat, high, preferred_element_type=jnp.float32) + jnp.dot(
            flat, low, preferred_element_type=jnp.float32
        )
        for p in range(2):
            blocks = [
                spectra[i * rows : (i + 1) * rows, p * LANES : (p + 1) * LANES]
                for i in range(ch_out)
            ]
            blocks = swap_blocks(blocks, AVG)
            for k in range(ch_out):
                start = p * half + th * LANES
                send1[k, :, start : start + LANES] = blocks[k].astype(jnp.bfloat16)

    pl.semaphore_wait(barrier, total - 1)

    def first_copy(off, mine):
        d = lax.rem(me + off, ns)
        return pltpu.make_async_remote_copy(
            src_ref=send1.at[d // spread],
            dst_ref=held.at[mine],
            send_sem=ssem1.at[off],
            recv_sem=rsem1.at[mine],
            device_id=(b, d),
            device_id_type=MESH,
        )

    offsets = sorted(range(1, ns), key=lambda o: abs(o - ns / 2))
    for off in offsets:
        first_copy(off, me).start()
    held[me] = send1[me // spread]

    def find_dev(g, carry):
        def body(s, acc):
            return jnp.where(god_ref[s] == g, s, acc)

        dev_of[g] = lax.fori_loop(0, ns, body, jnp.int32(0), unroll=min(ns, 8))
        return carry

    lax.fori_loop(0, ns, find_dev, 0)
    quarter = lax.rem(me, spread)

    def find_col(i, carry):
        g1 = quarter * ch_out + i // ns
        o = lax.rem(i, ns)

        def body(g2, acc):
            return jnp.where(own_ref[g1, g2] == o, dev_of[g2], acc)

        table[i] = lax.fori_loop(0, ns, body, jnp.int32(0), unroll=min(ns, 8))
        return carry

    lax.fori_loop(0, ch_out * ns, find_col, 0)

    for off in offsets:
        first_copy(off, lax.rem(me + ns - off, ns)).wait_recv()

    span = ch_out * rows
    for g in range(ch_out):
        x = held[dev_of[quarter * ch_out + g]]
        left[g * rows : (g + 1) * rows, :] = x
        left[span + g * rows : span + (g + 1) * rows, :half] = x[:, half:]
        left[span + g * rows : span + (g + 1) * rows, half:] = -x[:, :half]
    per_tile = LANES // rows
    lhs = left[...]
    for h in range(ns // per_tile):
        rhs = held[h * per_tile : (h + 1) * per_tile].reshape(LANES, 2 * half)
        block = lax.dot_general(
            lhs, rhs, (((1,), (1,)), ((), ())), preferred_element_type=jnp.float32
        )
        vis[h] = block * (1.0 / (AVG * spec))
    sub = rows // per_tile
    for h in range(ns // per_tile):
        blocks = [
            vis[h, pl.ds(q, 2 * span // per_tile, stride=per_tile), :] for q in range(per_tile)
        ]
        blocks = swap_blocks(blocks, rows)
        for s in range(per_tile):
            tiles[h * per_tile + s] = blocks[s].reshape(2 * ch_out, sub, LANES)

    def build(o, carry):
        for fl in range(fl_count):
            for g in range(rpf):
                row = fl * rpf + g
                source = table[row * ns + o]
                for p in range(2):
                    mixed[fl * ns + o, p, pl.ds(g, sub, stride=rpf), :] = tiles[
                        source, p * ch_out + row
                    ]
        return carry

    lax.fori_loop(0, ns, build, 0)

    def convert(i, carry):
        send2[i] = mixed[i].astype(jnp.bfloat16)
        return carry

    lax.fori_loop(0, fl_count * ns, convert, 0)

    channel = b * ch_out + me // spread

    def target(i):
        f = quarter * fl_count + lax.rem(b + i // ns, fl_count)
        o = lax.rem(me + i, ns)
        return f, o

    def second_copy(i):
        f, o = target(i)
        return pltpu.make_async_remote_copy(
            src_ref=send2.at[lax.rem(f, fl_count) * ns + o],
            dst_ref=out_ref.at[channel],
            send_sem=ssem2.at[i],
            recv_sem=rsem2.at[channel],
            device_id=(f, o),
            device_id_type=MESH,
        )

    own_here = quarter == b // fl_count

    def start_second(i, carry):
        second_copy(i).start()
        return carry

    def wait_second(i, carry):
        second_copy(i).wait_send()
        return carry

    pl.when(jnp.logical_not(own_here))(lambda: second_copy(0).start())
    lax.fori_loop(1, fl_count * ns, start_second, 0)

    @pl.when(own_here)
    def _():
        out_ref[channel] = send2[lax.rem(b, fl_count) * ns + me]

    for off in offsets:
        first_copy(off, me).wait_send()

    def arrived(slot):
        pltpu.make_async_remote_copy(
            src_ref=send2.at[0],
            dst_ref=out_ref.at[slot],
            send_sem=ssem2.at[0],
            recv_sem=rsem2.at[slot],
            device_id=(b, me),
            device_id_type=MESH,
        ).wait_recv()

    def wait_arrival(i, carry):
        arrived(lax.rem(channel + i, nf * ch_out))
        return carry

    pl.when(jnp.logical_not(own_here))(lambda: arrived(channel))
    lax.fori_loop(1, nf * ch_out, wait_arrival, 0)
    pl.when(jnp.logical_not(own_here))(lambda: second_copy(0).wait_send())
    lax.fori_loop(1, fl_count * ns, wait_second, 0)


def shards(nf, ns, samples, window, group_of_device, owner_map):
    _, rows, spec, _, length = samples.shape
    ch_out = length // AVG
    rpf = ns // nf
    fl_count = ch_out // rpf
    per_tile = LANES // rows
    sub = rows // per_tile
    depth = 2 * spec * AVG
    index = np.arange(length)
    theta = (index[:, None] * index[None, :] % length) * (2.0 * math.pi / length)
    cosine = jnp.asarray(np.cos(theta), jnp.float32)
    sine = jnp.asarray(np.sin(theta), jnp.float32)
    x = samples.reshape(rows * spec * 2, length)
    vmem = pl.BlockSpec(memory_space=pltpu.VMEM)
    smem = pl.BlockSpec(memory_space=pltpu.SMEM)
    out = pl.pallas_call(
        functools.partial(kernel, nf, ns, rows, spec),
        out_shape=jax.ShapeDtypeStruct((nf * ch_out, 2, sub * rpf, LANES), jnp.bfloat16),
        in_specs=[vmem, vmem, vmem, vmem, smem, smem],
        out_specs=vmem,
        scratch_shapes=[
            pltpu.VMEM((rows * spec * 2, length), jnp.float32),
            pltpu.VMEM((ch_out, rows, depth), jnp.bfloat16),
            pltpu.VMEM((ns, rows, depth), jnp.bfloat16),
            pltpu.VMEM((2 * ch_out * rows, depth), jnp.bfloat16),
            pltpu.VMEM((ns // per_tile, 2 * ch_out * rows, LANES), jnp.float32),
            pltpu.VMEM((ns, 2 * ch_out, sub, LANES), jnp.float32),
            pltpu.VMEM((fl_count * ns, 2, sub * rpf, LANES), jnp.float32),
            pltpu.VMEM((fl_count * ns, 2, sub * rpf, LANES), jnp.bfloat16),
            pltpu.SMEM((ns,), jnp.int32),
            pltpu.SMEM((ch_out * ns,), jnp.int32),
            pltpu.SemaphoreType.DMA((ns,)),
            pltpu.SemaphoreType.DMA((ns,)),
            pltpu.SemaphoreType.DMA((fl_count * ns,)),
            pltpu.SemaphoreType.DMA((nf * ch_out,)),
        ],
        compiler_params=pltpu.CompilerParams(collective_id=0, has_side_effects=True),
    )(x, window.reshape(1, length), cosine, sine, group_of_device, owner_map)
    out = out.reshape(nf * ch_out, 2, sub, rpf, LANES).transpose(1, 0, 3, 2, 4)
    return out.reshape(2, nf * ch_out, 1, rpf, rows * rows)


def solution(mesh):
    return jax.shard_map(
        functools.partial(shards, mesh.shape["freq"], mesh.shape["stn"]),
        mesh=mesh,
        in_specs=(P("freq", "stn", None, None, None), P(), P(), P()),
        out_specs=P(None, None, "stn", "freq", None),
        check_vma=False,
    )
```

```python
import functools
import math

import jax
import jax.numpy as jnp
import numpy as np
from jax import lax
from jax.experimental import pallas as pl
from jax.experimental.pallas import tpu as pltpu
from jax.sharding import PartitionSpec as P

AVG = 16
LANES = 128
MESH = pl.DeviceIdType.MESH
OUT_SPACE = pl.ANY


def swap_blocks(blocks, width):
    blocks = list(blocks)
    count = len(blocks)
    lane = lax.broadcasted_iota(jnp.int32, blocks[0].shape, 1) // width
    step = count // 2
    while step:
        upper = (lane // step) % 2 == 1
        for i in range(count):
            if (i // step) % 2 == 0:
                u, v = blocks[i], blocks[i + step]
                shift = step * width
                blocks[i] = jnp.where(upper, pltpu.roll(v, shift, 1), u)
                blocks[i + step] = jnp.where(upper, v, pltpu.roll(u, LANES - shift, 1))
        step //= 2
    return blocks


def kernel(
    nf, ns, rows, spec,
    x_hbm, w_hbm, trig_hbm, god_hbm, own_hbm,
    out_ref,
    x_ref, w_ref, trig_ref, god_ref, own_ref,
    xf, send1, held, left, vis, tiles, mixed, send2, dev_of, table,
    lsem, row_sem, ssem1, rsem1, ssem2, rsem2,
):
    length = LANES
    ch_out = length // AVG
    spread = ns // ch_out
    rpf = ns // nf
    fl_count = ch_out // rpf
    half = spec * AVG
    b = lax.axis_index("freq")
    me = lax.axis_index("stn")

    loads = [
        pltpu.make_async_copy(src, dst, lsem.at[n])
        for n, (src, dst) in enumerate(
            [
                (x_hbm, x_ref), (w_hbm, w_ref), (trig_hbm, trig_ref),
                (god_hbm, god_ref), (own_hbm, own_ref),
            ]
        )
    ]
    barrier = pltpu.get_barrier_semaphore()
    offsets = sorted(range(1, ns), key=lambda o: abs(o - ns / 2))
    for off in offsets:
        pl.semaphore_signal(
            barrier, inc=1, device_id=(b, lax.rem(me + off, ns)), device_id_type=MESH
        )
    for off in range(1, nf):
        pl.semaphore_signal(
            barrier, inc=1, device_id=(lax.rem(b + off, nf), me), device_id_type=MESH
        )
    for load in loads:
        load.start()
    for load in loads:
        load.wait()

    weights = jnp.broadcast_to(w_ref[...], (length, length)).T * (1.0 / math.sqrt(length))
    cosine = weights * trig_ref[0]
    sine = weights * trig_ref[1]
    matrix = jnp.concatenate(
        [jnp.concatenate([cosine, -sine], axis=1), jnp.concatenate([sine, cosine], axis=1)], axis=0
    )
    high = matrix.astype(jnp.bfloat16)
    low = (matrix - high.astype(jnp.float32)).astype(jnp.bfloat16)

    xf[...] = x_ref[...].astype(jnp.float32)
    for th in range(spec // ch_out):
        parts = []
        for t in range(th * ch_out, (th + 1) * ch_out):
            re = xf[pl.ds(2 * t, rows, stride=2 * spec), :]
            im = xf[pl.ds(2 * t + 1, rows, stride=2 * spec), :]
            parts.append(jnp.concatenate([re, im], axis=1).astype(jnp.bfloat16))
        flat = jnp.concatenate(parts, axis=0)
        spectra = jnp.dot(flat, high, preferred_element_type=jnp.float32) + jnp.dot(
            flat, low, preferred_element_type=jnp.float32
        )
        for p in range(2):
            blocks = [
                spectra[i * rows : (i + 1) * rows, p * LANES : (p + 1) * LANES]
                for i in range(ch_out)
            ]
            blocks = swap_blocks(blocks, AVG)
            for k in range(ch_out):
                start = p * half + th * LANES
                send1[k, :, start : start + LANES] = blocks[k].astype(jnp.bfloat16)

    pl.semaphore_wait(barrier, ns - 1 + nf - 1)

    def first_copy(off, mine):
        d = lax.rem(me + off, ns)
        return pltpu.make_async_remote_copy(
            src_ref=send1.at[d // spread],
            dst_ref=held.at[mine],
            send_sem=ssem1.at[off],
            recv_sem=rsem1.at[mine],
            device_id=(b, d),
            device_id_type=MESH,
        )

    for off in offsets:
        first_copy(off, me).start()
    for off in range(1, nf):
        pl.semaphore_signal(
            row_sem, inc=1, device_id=(lax.rem(b + off, nf), me), device_id_type=MESH
        )
    held[me] = send1[me // spread]

    def find_dev(g, carry):
        def body(s, acc):
            return jnp.where(god_ref[s] == g, s, acc)

        dev_of[g] = lax.fori_loop(0, ns, body, jnp.int32(0), unroll=min(ns, 8))
        return carry

    lax.fori_loop(0, ns, find_dev, 0)
    quarter = lax.rem(me, spread)

    def find_col(i, carry):
        g1 = quarter * ch_out + i // ns
        o = lax.rem(i, ns)

        def body(g2, acc):
            return jnp.where(own_ref[g1, g2] == o, dev_of[g2], acc)

        table[i] = lax.fori_loop(0, ns, body, jnp.int32(0), unroll=min(ns, 8))
        return carry

    lax.fori_loop(0, ch_out * ns, find_col, 0)
    pl.semaphore_wait(row_sem, nf - 1)

    for off in offsets:
        first_copy(off, lax.rem(me + ns - off, ns)).wait_recv()

    channel = b * ch_out + me // spread
    own_here = quarter == b // fl_count

    def second_copy(df, step):
        f = quarter * fl_count + lax.rem(b + df, fl_count)
        o = lax.rem(me + step, ns)
        return pltpu.make_async_remote_copy(
            src_ref=send2.at[df * ns + o],
            dst_ref=out_ref.at[:, channel],
            send_sem=ssem2.at[df * ns + step],
            recv_sem=rsem2.at[channel],
            device_id=(f, o),
            device_id_type=MESH,
        )

    per_tile = LANES // rows
    sub = rows // per_tile
    span = rpf * rows
    for df in range(fl_count):
        fl = lax.rem(b + df, fl_count)
        for g in range(rpf):
            x = held[dev_of[quarter * ch_out + fl * rpf + g]]
            left[g * rows : (g + 1) * rows, :] = x
            left[span + g * rows : span + (g + 1) * rows, :half] = x[:, half:]
            left[span + g * rows : span + (g + 1) * rows, half:] = -x[:, :half]
        lhs = left[...]
        for h in range(ns // per_tile):
            rhs = held[h * per_tile : (h + 1) * per_tile].reshape(LANES, 2 * half)
            block = lax.dot_general(
                lhs, rhs, (((1,), (1,)), ((), ())), preferred_element_type=jnp.float32
            )
            vis[h] = block * (1.0 / (AVG * spec))
            blocks = [
                vis[h, pl.ds(q, 2 * span // per_tile, stride=per_tile), :] for q in range(per_tile)
            ]
            blocks = swap_blocks(blocks, rows)
            for s in range(per_tile):
                tiles[h * per_tile + s] = blocks[s].reshape(2 * rpf, sub, LANES)

        def build(o, carry):
            for g in range(rpf):
                source = table[(fl * rpf + g) * ns + o]
                for p in range(2):
                    mixed[o, p, pl.ds(g, sub, stride=rpf), :] = tiles[source, p * rpf + g]
            for p in range(2):
                for r in range(sub):
                    send2[df * ns + o, p, :, r * LANES : (r + 1) * LANES] = mixed[
                        o, p, r * rpf : (r + 1) * rpf, :
                    ].astype(jnp.bfloat16)
            return carry

        lax.fori_loop(0, ns, build, 0, unroll=min(ns, 8))

        for off in offsets:
            second_copy(df, off).start()
        if df:
            second_copy(df, 0).start()
        else:
            pl.when(jnp.logical_not(own_here))(lambda: second_copy(0, 0).start())

    @pl.when(own_here)
    def _():
        own = pltpu.make_async_copy(send2.at[me], out_ref.at[:, channel], lsem.at[0])
        own.start()
        own.wait()

    for off in offsets:
        first_copy(off, me).wait_send()

    def arrived(slot):
        pltpu.make_async_remote_copy(
            src_ref=send2.at[0],
            dst_ref=out_ref.at[:, slot],
            send_sem=ssem2.at[0],
            recv_sem=rsem2.at[slot],
            device_id=(b, me),
            device_id_type=MESH,
        ).wait_recv()

    def wait_arrival(i, carry):
        arrived(lax.rem(channel + i, nf * ch_out))
        return carry

    pl.when(jnp.logical_not(own_here))(lambda: arrived(channel))
    lax.fori_loop(1, nf * ch_out, wait_arrival, 0)

    def wait_second(i, carry):
        second_copy(i // ns, lax.rem(i, ns)).wait_send()
        return carry

    pl.when(jnp.logical_not(own_here))(lambda: second_copy(0, 0).wait_send())
    lax.fori_loop(1, fl_count * ns, wait_second, 0)


def shards(nf, ns, samples, window, group_of_device, owner_map):
    _, rows, spec, _, length = samples.shape
    ch_out = length // AVG
    rpf = ns // nf
    fl_count = ch_out // rpf
    per_tile = LANES // rows
    sub = rows // per_tile
    depth = 2 * spec * AVG
    index = np.arange(length)
    theta = (index[:, None] * index[None, :] % length) * (2.0 * math.pi / length)
    trig = jnp.asarray(np.stack([np.cos(theta), np.sin(theta)]), jnp.float32)
    x = samples.reshape(rows * spec * 2, length)
    hbm = pl.BlockSpec(memory_space=pltpu.HBM)
    out = pl.pallas_call(
        functools.partial(kernel, nf, ns, rows, spec),
        out_shape=jax.ShapeDtypeStruct((2, nf * ch_out, rpf, sub * LANES), jnp.bfloat16),
        in_specs=[hbm] * 5,
        out_specs=pl.BlockSpec(memory_space=OUT_SPACE),
        scratch_shapes=[
            pltpu.VMEM((rows * spec * 2, length), jnp.bfloat16),
            pltpu.VMEM((1, length), jnp.float32),
            pltpu.VMEM((2, length, length), jnp.float32),
            pltpu.SMEM((ns,), jnp.int32),
            pltpu.SMEM((ns, ns), jnp.int32),
            pltpu.VMEM((rows * spec * 2, length), jnp.float32),
            pltpu.VMEM((ch_out, rows, depth), jnp.bfloat16),
            pltpu.VMEM((ns, rows, depth), jnp.bfloat16),
            pltpu.VMEM((2 * rpf * rows, depth), jnp.bfloat16),
            pltpu.VMEM((ns // per_tile, 2 * rpf * rows, LANES), jnp.float32),
            pltpu.VMEM((ns, 2 * rpf, sub, LANES), jnp.float32),
            pltpu.VMEM((ns, 2, sub * rpf, LANES), jnp.float32),
            pltpu.VMEM((fl_count * ns, 2, rpf, sub * LANES), jnp.bfloat16),
            pltpu.SMEM((ns,), jnp.int32),
            pltpu.SMEM((ch_out * ns,), jnp.int32),
            pltpu.SemaphoreType.DMA((5,)),
            pltpu.SemaphoreType.REGULAR,
            pltpu.SemaphoreType.DMA((ns,)),
            pltpu.SemaphoreType.DMA((ns,)),
            pltpu.SemaphoreType.DMA((fl_count * ns,)),
            pltpu.SemaphoreType.DMA((nf * ch_out,)),
        ],
        compiler_params=pltpu.CompilerParams(
            collective_id=0, has_side_effects=True, vmem_limit_bytes=60 * 1024 * 1024
        ),
    )(x, window.reshape(1, length), trig, group_of_device, owner_map)
    return out[:, :, None]


def solution(mesh):
    return jax.shard_map(
        functools.partial(shards, mesh.shape["freq"], mesh.shape["stn"]),
        mesh=mesh,
        in_specs=(P("freq", "stn", None, None, None), P(), P(), P()),
        out_specs=P(None, None, "stn", "freq", None),
        check_vma=False,
    )
```

```python
import functools
import math

import jax
import jax.numpy as jnp
import numpy as np
from jax import lax
from jax.experimental import pallas as pl
from jax.experimental.pallas import tpu as pltpu
from jax.sharding import PartitionSpec as P

AVG = 16
LANES = 128
MESH = pl.DeviceIdType.MESH
OUT_SPACE = pltpu.VMEM


def swap_blocks(blocks, width):
    blocks = list(blocks)
    count = len(blocks)
    lane = lax.broadcasted_iota(jnp.int32, blocks[0].shape, 1) // width
    step = count // 2
    while step:
        upper = (lane // step) % 2 == 1
        for i in range(count):
            if (i // step) % 2 == 0:
                u, v = blocks[i], blocks[i + step]
                shift = step * width
                blocks[i] = jnp.where(upper, pltpu.roll(v, shift, 1), u)
                blocks[i + step] = jnp.where(upper, v, pltpu.roll(u, LANES - shift, 1))
        step //= 2
    return blocks


def kernel(
    nf, ns, rows, spec,
    x_hbm, w_hbm, trig_hbm, god_hbm, own_hbm,
    out_ref,
    x_ref, w_ref, trig_ref, god_ref, own_ref,
    xf, send1, held, left, vis, tiles, mixed, send2, dev_of, table,
    lsem, row_sem, ssem1, rsem1, ssem2, rsem2,
):
    length = LANES
    ch_out = length // AVG
    spread = ns // ch_out
    rpf = ns // nf
    fl_count = ch_out // rpf
    half = spec * AVG
    b = lax.axis_index("freq")
    me = lax.axis_index("stn")

    loads = [
        pltpu.make_async_copy(src, dst, lsem.at[n])
        for n, (src, dst) in enumerate(
            [
                (x_hbm, x_ref), (w_hbm, w_ref), (trig_hbm, trig_ref),
                (god_hbm, god_ref), (own_hbm, own_ref),
            ]
        )
    ]
    barrier = pltpu.get_barrier_semaphore()
    offsets = sorted(range(1, ns), key=lambda o: abs(o - ns / 2))
    for off in offsets:
        pl.semaphore_signal(
            barrier, inc=1, device_id=(b, lax.rem(me + off, ns)), device_id_type=MESH
        )
    for off in range(1, nf):
        pl.semaphore_signal(
            barrier, inc=1, device_id=(lax.rem(b + off, nf), me), device_id_type=MESH
        )
    for load in loads:
        load.start()
    for load in loads:
        load.wait()

    weights = jnp.broadcast_to(w_ref[...], (length, length)).T * (1.0 / math.sqrt(length))
    cosine = weights * trig_ref[0]
    sine = weights * trig_ref[1]
    matrix = jnp.concatenate(
        [jnp.concatenate([cosine, -sine], axis=1), jnp.concatenate([sine, cosine], axis=1)], axis=0
    )
    high = matrix.astype(jnp.bfloat16)
    low = (matrix - high.astype(jnp.float32)).astype(jnp.bfloat16)

    xf[...] = x_ref[...].astype(jnp.float32)
    for th in range(spec // ch_out):
        parts = []
        for t in range(th * ch_out, (th + 1) * ch_out):
            re = xf[pl.ds(2 * t, rows, stride=2 * spec), :]
            im = xf[pl.ds(2 * t + 1, rows, stride=2 * spec), :]
            parts.append(jnp.concatenate([re, im], axis=1).astype(jnp.bfloat16))
        flat = jnp.concatenate(parts, axis=0)
        spectra = jnp.dot(flat, high, preferred_element_type=jnp.float32) + jnp.dot(
            flat, low, preferred_element_type=jnp.float32
        )
        for p in range(2):
            blocks = [
                spectra[i * rows : (i + 1) * rows, p * LANES : (p + 1) * LANES]
                for i in range(ch_out)
            ]
            blocks = swap_blocks(blocks, AVG)
            for k in range(ch_out):
                start = p * half + th * LANES
                send1[k, :, start : start + LANES] = blocks[k].astype(jnp.bfloat16)

    pl.semaphore_wait(barrier, ns - 1 + nf - 1)

    def first_copy(off, mine):
        d = lax.rem(me + off, ns)
        return pltpu.make_async_remote_copy(
            src_ref=send1.at[d // spread],
            dst_ref=held.at[mine],
            send_sem=ssem1.at[off],
            recv_sem=rsem1.at[mine],
            device_id=(b, d),
            device_id_type=MESH,
        )

    for off in offsets:
        first_copy(off, me).start()
    for off in range(1, nf):
        pl.semaphore_signal(
            row_sem, inc=1, device_id=(lax.rem(b + off, nf), me), device_id_type=MESH
        )
    held[me] = send1[me // spread]

    def find_dev(g, carry):
        def body(s, acc):
            return jnp.where(god_ref[s] == g, s, acc)

        dev_of[g] = lax.fori_loop(0, ns, body, jnp.int32(0), unroll=min(ns, 8))
        return carry

    lax.fori_loop(0, ns, find_dev, 0)
    quarter = lax.rem(me, spread)

    def find_col(i, carry):
        g1 = quarter * ch_out + i // ns
        o = lax.rem(i, ns)

        def body(g2, acc):
            return jnp.where(own_ref[g1, g2] == o, dev_of[g2], acc)

        table[i] = lax.fori_loop(0, ns, body, jnp.int32(0), unroll=min(ns, 8))
        return carry

    lax.fori_loop(0, ch_out * ns, find_col, 0)
    pl.semaphore_wait(row_sem, nf - 1)

    for off in offsets:
        first_copy(off, lax.rem(me + ns - off, ns)).wait_recv()

    channel = b * ch_out + me // spread
    own_here = quarter == b // fl_count

    def second_copy(df, step):
        f = quarter * fl_count + lax.rem(b + df, fl_count)
        o = lax.rem(me + step, ns)
        return pltpu.make_async_remote_copy(
            src_ref=send2.at[df * ns + o],
            dst_ref=out_ref.at[:, channel],
            send_sem=ssem2.at[df * ns + step],
            recv_sem=rsem2.at[channel],
            device_id=(f, o),
            device_id_type=MESH,
        )

    per_tile = LANES // rows
    sub = rows // per_tile
    span = rpf * rows
    for df in range(fl_count):
        fl = lax.rem(b + df, fl_count)
        for g in range(rpf):
            x = held[dev_of[quarter * ch_out + fl * rpf + g]]
            left[g * rows : (g + 1) * rows, :] = x
            left[span + g * rows : span + (g + 1) * rows, :half] = x[:, half:]
            left[span + g * rows : span + (g + 1) * rows, half:] = -x[:, :half]
        lhs = left[...]
        for h in range(ns // per_tile):
            rhs = held[h * per_tile : (h + 1) * per_tile].reshape(LANES, 2 * half)
            block = lax.dot_general(
                lhs, rhs, (((1,), (1,)), ((), ())), preferred_element_type=jnp.float32
            )
            vis[h] = block * (1.0 / (AVG * spec))
            blocks = [
                vis[h, pl.ds(q, 2 * span // per_tile, stride=per_tile), :] for q in range(per_tile)
            ]
            blocks = swap_blocks(blocks, rows)
            for s in range(per_tile):
                tiles[h * per_tile + s] = blocks[s].reshape(2 * rpf, sub, LANES)

        def build(o, carry):
            for g in range(rpf):
                source = table[(fl * rpf + g) * ns + o]
                for p in range(2):
                    mixed[o, p, pl.ds(g, sub, stride=rpf), :] = tiles[source, p * rpf + g]
            for p in range(2):
                for r in range(sub):
                    send2[df * ns + o, p, :, r * LANES : (r + 1) * LANES] = mixed[
                        o, p, r * rpf : (r + 1) * rpf, :
                    ].astype(jnp.bfloat16)
            return carry

        lax.fori_loop(0, ns, build, 0, unroll=min(ns, 8))

        for off in offsets:
            second_copy(df, off).start()
        if df:
            second_copy(df, 0).start()
        else:
            pl.when(jnp.logical_not(own_here))(lambda: second_copy(0, 0).start())

    @pl.when(own_here)
    def _():
        own = pltpu.make_async_copy(send2.at[me], out_ref.at[:, channel], lsem.at[0])
        own.start()
        own.wait()

    for off in offsets:
        first_copy(off, me).wait_send()

    def arrived(slot):
        pltpu.make_async_remote_copy(
            src_ref=send2.at[0],
            dst_ref=out_ref.at[:, slot],
            send_sem=ssem2.at[0],
            recv_sem=rsem2.at[slot],
            device_id=(b, me),
            device_id_type=MESH,
        ).wait_recv()

    def wait_arrival(i, carry):
        arrived(lax.rem(channel + i, nf * ch_out))
        return carry

    pl.when(jnp.logical_not(own_here))(lambda: arrived(channel))
    lax.fori_loop(1, nf * ch_out, wait_arrival, 0)

    def wait_second(i, carry):
        second_copy(i // ns, lax.rem(i, ns)).wait_send()
        return carry

    pl.when(jnp.logical_not(own_here))(lambda: second_copy(0, 0).wait_send())
    lax.fori_loop(1, fl_count * ns, wait_second, 0)


def shards(nf, ns, samples, window, group_of_device, owner_map):
    _, rows, spec, _, length = samples.shape
    ch_out = length // AVG
    rpf = ns // nf
    fl_count = ch_out // rpf
    per_tile = LANES // rows
    sub = rows // per_tile
    depth = 2 * spec * AVG
    index = np.arange(length)
    theta = (index[:, None] * index[None, :] % length) * (2.0 * math.pi / length)
    trig = jnp.asarray(np.stack([np.cos(theta), np.sin(theta)]), jnp.float32)
    x = samples.reshape(rows * spec * 2, length)
    hbm = pl.BlockSpec(memory_space=pltpu.HBM)
    out = pl.pallas_call(
        functools.partial(kernel, nf, ns, rows, spec),
        out_shape=pltpu.VMEM((2, nf * ch_out, rpf, sub * LANES), jnp.bfloat16),
        in_specs=[hbm] * 5,
        out_specs=pl.BlockSpec(memory_space=OUT_SPACE),
        scratch_shapes=[
            pltpu.VMEM((rows * spec * 2, length), jnp.bfloat16),
            pltpu.VMEM((1, length), jnp.float32),
            pltpu.VMEM((2, length, length), jnp.float32),
            pltpu.SMEM((ns,), jnp.int32),
            pltpu.SMEM((ns, ns), jnp.int32),
            pltpu.VMEM((rows * spec * 2, length), jnp.float32),
            pltpu.VMEM((ch_out, rows, depth), jnp.bfloat16),
            pltpu.VMEM((ns, rows, depth), jnp.bfloat16),
            pltpu.VMEM((2 * rpf * rows, depth), jnp.bfloat16),
            pltpu.VMEM((ns // per_tile, 2 * rpf * rows, LANES), jnp.float32),
            pltpu.VMEM((ns, 2 * rpf, sub, LANES), jnp.float32),
            pltpu.VMEM((ns, 2, sub * rpf, LANES), jnp.float32),
            pltpu.VMEM((fl_count * ns, 2, rpf, sub * LANES), jnp.bfloat16),
            pltpu.SMEM((ns,), jnp.int32),
            pltpu.SMEM((ch_out * ns,), jnp.int32),
            pltpu.SemaphoreType.DMA((5,)),
            pltpu.SemaphoreType.REGULAR,
            pltpu.SemaphoreType.DMA((ns,)),
            pltpu.SemaphoreType.DMA((ns,)),
            pltpu.SemaphoreType.DMA((fl_count * ns,)),
            pltpu.SemaphoreType.DMA((nf * ch_out,)),
        ],
        compiler_params=pltpu.CompilerParams(
            collective_id=0, has_side_effects=True, vmem_limit_bytes=60 * 1024 * 1024
        ),
    )(x, window.reshape(1, length), trig, group_of_device, owner_map)
    return out[:, :, None]


def solution(mesh):
    return jax.shard_map(
        functools.partial(shards, mesh.shape["freq"], mesh.shape["stn"]),
        mesh=mesh,
        in_specs=(P("freq", "stn", None, None, None), P(), P(), P()),
        out_specs=P(None, None, "stn", "freq", None),
        check_vma=False,
    )
```

```python
import functools
import math

import jax
import jax.numpy as jnp
import numpy as np
from jax import lax
from jax.experimental import pallas as pl
from jax.experimental.pallas import tpu as pltpu
from jax.sharding import PartitionSpec as P

AVG = 16
LANES = 128
MESH = pl.DeviceIdType.MESH
OUT_SPACE = pltpu.VMEM


def swap_blocks(blocks, width):
    blocks = list(blocks)
    count = len(blocks)
    lane = lax.broadcasted_iota(jnp.int32, blocks[0].shape, 1) // width
    step = count // 2
    while step:
        upper = (lane // step) % 2 == 1
        for i in range(count):
            if (i // step) % 2 == 0:
                u, v = blocks[i], blocks[i + step]
                shift = step * width
                blocks[i] = jnp.where(upper, pltpu.roll(v, shift, 1), u)
                blocks[i + step] = jnp.where(upper, v, pltpu.roll(u, LANES - shift, 1))
        step //= 2
    return blocks


def kernel(
    nf, ns, rows, spec,
    x_hbm, w_hbm, trig_hbm, god_hbm, own_hbm,
    out_ref,
    x_ref, w_ref, trig_ref, god_ref, own_ref,
    xf, send1, held, left, vis, tiles, mixed, send2, dev_of, table,
    lsem, row_sem, ssem1, rsem1, ssem2, rsem2,
):
    length = LANES
    ch_out = length // AVG
    spread = ns // ch_out
    rpf = ns // nf
    fl_count = ch_out // rpf
    half = spec * AVG
    b = lax.axis_index("freq")
    me = lax.axis_index("stn")

    loads = [
        pltpu.make_async_copy(src, dst, lsem.at[n])
        for n, (src, dst) in enumerate(
            [
                (x_hbm, x_ref), (w_hbm, w_ref), (trig_hbm, trig_ref),
                (god_hbm, god_ref), (own_hbm, own_ref),
            ]
        )
    ]
    barrier = pltpu.get_barrier_semaphore()
    offsets = sorted(range(1, ns), key=lambda o: abs(o - ns / 2))
    for off in offsets:
        pl.semaphore_signal(
            barrier, inc=1, device_id=(b, lax.rem(me + off, ns)), device_id_type=MESH
        )
    for off in range(1, nf):
        pl.semaphore_signal(
            barrier, inc=1, device_id=(lax.rem(b + off, nf), me), device_id_type=MESH
        )
    for load in loads:
        load.start()
    for load in loads:
        load.wait()

    weights = jnp.broadcast_to(w_ref[...], (length, length)).T * (1.0 / math.sqrt(length))
    cosine = weights * trig_ref[0]
    sine = weights * trig_ref[1]
    matrix = jnp.concatenate(
        [jnp.concatenate([cosine, -sine], axis=1), jnp.concatenate([sine, cosine], axis=1)], axis=0
    )
    high = matrix.astype(jnp.bfloat16)
    low = (matrix - high.astype(jnp.float32)).astype(jnp.bfloat16)

    xf[...] = x_ref[...].astype(jnp.float32)
    for th in range(spec // ch_out):
        parts = []
        for t in range(th * ch_out, (th + 1) * ch_out):
            re = xf[pl.ds(2 * t, rows, stride=2 * spec), :]
            im = xf[pl.ds(2 * t + 1, rows, stride=2 * spec), :]
            parts.append(jnp.concatenate([re, im], axis=1).astype(jnp.bfloat16))
        flat = jnp.concatenate(parts, axis=0)
        spectra = jnp.dot(flat, high, preferred_element_type=jnp.float32) + jnp.dot(
            flat, low, preferred_element_type=jnp.float32
        )
        for p in range(2):
            blocks = [
                spectra[i * rows : (i + 1) * rows, p * LANES : (p + 1) * LANES]
                for i in range(ch_out)
            ]
            blocks = swap_blocks(blocks, AVG)
            for k in range(ch_out):
                start = p * half + th * LANES
                send1[k, :, start : start + LANES] = blocks[k].astype(jnp.bfloat16)

    pl.semaphore_wait(barrier, ns - 1 + nf - 1)

    def first_copy(off, mine):
        d = lax.rem(me + off, ns)
        return pltpu.make_async_remote_copy(
            src_ref=send1.at[d // spread],
            dst_ref=held.at[mine],
            send_sem=ssem1.at[off],
            recv_sem=rsem1.at[mine],
            device_id=(b, d),
            device_id_type=MESH,
        )

    for off in offsets:
        first_copy(off, me).start()
    for off in range(1, nf):
        pl.semaphore_signal(
            row_sem, inc=1, device_id=(lax.rem(b + off, nf), me), device_id_type=MESH
        )
    held[me] = send1[me // spread]

    def find_dev(g, carry):
        def body(s, acc):
            return jnp.where(god_ref[s] == g, s, acc)

        dev_of[g] = lax.fori_loop(0, ns, body, jnp.int32(0), unroll=min(ns, 8))
        return carry

    lax.fori_loop(0, ns, find_dev, 0)
    quarter = lax.rem(me, spread)

    def find_col(i, carry):
        g1 = quarter * ch_out + i // ns
        o = lax.rem(i, ns)

        def body(g2, acc):
            return jnp.where(own_ref[g1, g2] == o, dev_of[g2], acc)

        table[i] = lax.fori_loop(0, ns, body, jnp.int32(0), unroll=min(ns, 8))
        return carry

    lax.fori_loop(0, ch_out * ns, find_col, 0)
    pl.semaphore_wait(row_sem, nf - 1)

    for off in offsets:
        first_copy(off, lax.rem(me + ns - off, ns)).wait_recv()

    channel = b * ch_out + me // spread
    own_here = quarter == b // fl_count

    def second_copy(df, step):
        f = quarter * fl_count + lax.rem(b + df + 1, fl_count)
        o = lax.rem(me + step, ns)
        return pltpu.make_async_remote_copy(
            src_ref=send2.at[df * ns + o],
            dst_ref=out_ref.at[:, channel],
            send_sem=ssem2.at[df * ns + step],
            recv_sem=rsem2.at[channel],
            device_id=(f, o),
            device_id_type=MESH,
        )

    per_tile = LANES // rows
    sub = rows // per_tile
    span = rpf * rows
    for df in range(fl_count):
        fl = lax.rem(b + df + 1, fl_count)
        for g in range(rpf):
            x = held[dev_of[quarter * ch_out + fl * rpf + g]]
            left[g * rows : (g + 1) * rows, :] = x
            left[span + g * rows : span + (g + 1) * rows, :half] = x[:, half:]
            left[span + g * rows : span + (g + 1) * rows, half:] = -x[:, :half]
        lhs = left[...]
        for h in range(ns // per_tile):
            rhs = held[h * per_tile : (h + 1) * per_tile].reshape(LANES, 2 * half)
            block = lax.dot_general(
                lhs, rhs, (((1,), (1,)), ((), ())), preferred_element_type=jnp.float32
            )
            vis[h] = block * (1.0 / (AVG * spec))
            blocks = [
                vis[h, pl.ds(q, 2 * span // per_tile, stride=per_tile), :] for q in range(per_tile)
            ]
            blocks = swap_blocks(blocks, rows)
            for s in range(per_tile):
                tiles[h * per_tile + s] = blocks[s].reshape(2 * rpf, sub, LANES)

        def build(o, carry):
            for g in range(rpf):
                source = table[(fl * rpf + g) * ns + o]
                for p in range(2):
                    mixed[o, p, pl.ds(g, sub, stride=rpf), :] = tiles[source, p * rpf + g]
            for p in range(2):
                for r in range(sub):
                    send2[df * ns + o, p, :, r * LANES : (r + 1) * LANES] = mixed[
                        o, p, r * rpf : (r + 1) * rpf, :
                    ].astype(jnp.bfloat16)
            return carry

        lax.fori_loop(0, ns, build, 0, unroll=min(ns, 8))

        for off in reversed(offsets):
            second_copy(df, off).start()
        if df != fl_count - 1:
            second_copy(df, 0).start()
        else:
            pl.when(jnp.logical_not(own_here))(lambda: second_copy(fl_count - 1, 0).start())

    @pl.when(own_here)
    def _():
        own = pltpu.make_async_copy(send2.at[(fl_count - 1) * ns + me], out_ref.at[:, channel], lsem.at[0])
        own.start()
        own.wait()

    for off in offsets:
        first_copy(off, me).wait_send()

    def arrived(slot):
        pltpu.make_async_remote_copy(
            src_ref=send2.at[0],
            dst_ref=out_ref.at[:, slot],
            send_sem=ssem2.at[0],
            recv_sem=rsem2.at[slot],
            device_id=(b, me),
            device_id_type=MESH,
        ).wait_recv()

    def wait_arrival(i, carry):
        arrived(lax.rem(channel + i, nf * ch_out))
        return carry

    pl.when(jnp.logical_not(own_here))(lambda: arrived(channel))
    lax.fori_loop(1, nf * ch_out, wait_arrival, 0)

    def wait_second(i, carry):
        second_copy(i // ns, lax.rem(i, ns)).wait_send()
        return carry

    pl.when(jnp.logical_not(own_here))(lambda: second_copy(fl_count - 1, 0).wait_send())
    lax.fori_loop(0, (fl_count - 1) * ns, wait_second, 0)
    lax.fori_loop((fl_count - 1) * ns + 1, fl_count * ns, wait_second, 0)


def shards(nf, ns, samples, window, group_of_device, owner_map):
    _, rows, spec, _, length = samples.shape
    ch_out = length // AVG
    rpf = ns // nf
    fl_count = ch_out // rpf
    per_tile = LANES // rows
    sub = rows // per_tile
    depth = 2 * spec * AVG
    index = np.arange(length)
    theta = (index[:, None] * index[None, :] % length) * (2.0 * math.pi / length)
    trig = jnp.asarray(np.stack([np.cos(theta), np.sin(theta)]), jnp.float32)
    x = samples.reshape(rows * spec * 2, length)
    hbm = pl.BlockSpec(memory_space=pltpu.HBM)
    out = pl.pallas_call(
        functools.partial(kernel, nf, ns, rows, spec),
        out_shape=pltpu.VMEM((2, nf * ch_out, rpf, sub * LANES), jnp.bfloat16),
        in_specs=[hbm] * 5,
        out_specs=pl.BlockSpec(memory_space=OUT_SPACE),
        scratch_shapes=[
            pltpu.VMEM((rows * spec * 2, length), jnp.bfloat16),
            pltpu.VMEM((1, length), jnp.float32),
            pltpu.VMEM((2, length, length), jnp.float32),
            pltpu.SMEM((ns,), jnp.int32),
            pltpu.SMEM((ns, ns), jnp.int32),
            pltpu.VMEM((rows * spec * 2, length), jnp.float32),
            pltpu.VMEM((ch_out, rows, depth), jnp.bfloat16),
            pltpu.VMEM((ns, rows, depth), jnp.bfloat16),
            pltpu.VMEM((2 * rpf * rows, depth), jnp.bfloat16),
            pltpu.VMEM((ns // per_tile, 2 * rpf * rows, LANES), jnp.float32),
            pltpu.VMEM((ns, 2 * rpf, sub, LANES), jnp.float32),
            pltpu.VMEM((ns, 2, sub * rpf, LANES), jnp.float32),
            pltpu.VMEM((fl_count * ns, 2, rpf, sub * LANES), jnp.bfloat16),
            pltpu.SMEM((ns,), jnp.int32),
            pltpu.SMEM((ch_out * ns,), jnp.int32),
            pltpu.SemaphoreType.DMA((5,)),
            pltpu.SemaphoreType.REGULAR,
            pltpu.SemaphoreType.DMA((ns,)),
            pltpu.SemaphoreType.DMA((ns,)),
            pltpu.SemaphoreType.DMA((fl_count * ns,)),
            pltpu.SemaphoreType.DMA((nf * ch_out,)),
        ],
        compiler_params=pltpu.CompilerParams(
            collective_id=0, has_side_effects=True, vmem_limit_bytes=60 * 1024 * 1024
        ),
    )(x, window.reshape(1, length), trig, group_of_device, owner_map)
    return out[:, :, None]


def solution(mesh):
    return jax.shard_map(
        functools.partial(shards, mesh.shape["freq"], mesh.shape["stn"]),
        mesh=mesh,
        in_specs=(P("freq", "stn", None, None, None), P(), P(), P()),
        out_specs=P(None, None, "stn", "freq", None),
        check_vma=False,
    )
```
